64 devices in a mesh: rep: 4 (over x, y), dp: 16 (over z, core).
Axes of the slice: x: 2, y: 2, z: 8, core: 2. Of those that a mesh axis runs over, the one named last changes fastest.
The devices are a block of a 4x4x8 slice.
Arguments:
- x: bfloat16 [64, 2048, 512], P(('rep', 'dp')), parts along dimension 0
- dy: bfloat16 [64, 2048, 512], P(('rep', 'dp')), parts along dimension 0
- wq: bfloat16 [2, 512, 1024], P(None, 'dp')
- wk: bfloat16 [2, 512, 512], P(None, 'dp')
- wv: bfloat16 [2, 512, 512], P(None, 'dp')
- wo: bfloat16 [2, 1024, 512], P(None, 'dp')
- w_gate: bfloat16 [2, 512, 1536], P(None, 'dp')
- w_up: bfloat16 [2, 512, 1536], P(None, 'dp')
- w_down: bfloat16 [2, 1536, 512], P(None, 'dp')
- m_wq: float32 [2, 512, 1024], P(None, 'dp')
- m_wk: float32 [2, 512, 512], P(None, 'dp')
- m_wv: float32 [2, 512, 512], P(None, 'dp')
- m_wo: float32 [2, 1024, 512], P(None, 'dp')
- m_w_gate: float32 [2, 512, 1536], P(None, 'dp')
- m_w_up: float32 [2, 512, 1536], P(None, 'dp')
- m_w_down: float32 [2, 1536, 512], P(None, 'dp')
- v_wq: float32 [2, 512, 1024], P(None, 'dp')
- v_wk: float32 [2, 512, 512], P(None, 'dp')
- v_wv: float32 [2, 512, 512], P(None, 'dp')
- v_wo: float32 [2, 1024, 512], P(None, 'dp')
- v_w_gate: float32 [2, 512, 1536], P(None, 'dp')
- v_w_up: float32 [2, 512, 1536], P(None, 'dp')
- v_w_down: float32 [2, 1536, 512], P(None, 'dp')
Outputs:
- output 1: bfloat16 [8, 512, 1024], P('rep', 'dp'), parts along dimension 0
- output 2: bfloat16 [8, 512, 512], P('rep', 'dp'), parts along dimension 0
- output 3: bfloat16 [8, 512, 512], P('rep', 'dp'), parts along dimension 0
- output 4: bfloat16 [8, 1024, 512], P('rep', 'dp'), parts along dimension 0
- output 5: bfloat16 [8, 512, 1536], P('rep', 'dp'), parts along dimension 0
- output 6: bfloat16 [8, 512, 1536], P('rep', 'dp'), parts along dimension 0
- output 7: bfloat16 [8, 1536, 512], P('rep', 'dp'), parts along dimension 0
- output 8: float32 [8, 512, 1024], P('rep', 'dp'), parts along dimension 0
- output 9: float32 [8, 512, 512], P('rep', 'dp'), parts along dimension 0
- output 10: float32 [8, 512, 512], P('rep', 'dp'), parts along dimension 0
- output 11: float32 [8, 1024, 512], P('rep', 'dp'), parts along dimension 0
- output 12: float32 [8, 512, 1536], P('rep', 'dp'), parts along dimension 0
- output 13: float32 [8, 512, 1536], P('rep', 'dp'), parts along dimension 0
- output 14: float32 [8, 1536, 512], P('rep', 'dp'), parts along dimension 0
- output 15: float32 [8, 512, 1024], P('rep', 'dp'), parts along dimension 0
- output 16: float32 [8, 512, 512], P('rep', 'dp'), parts along dimension 0
- output 17: float32 [8, 512, 512], P('rep', 'dp'), parts along dimension 0
- output 18: float32 [8, 1024, 512], P('rep', 'dp'), parts along dimension 0
- output 19: float32 [8, 512, 1536], P('rep', 'dp'), parts along dimension 0
- output 20: float32 [8, 512, 1536], P('rep', 'dp'), parts along dimension 0
- output 21: float32 [8, 1536, 512], P('rep', 'dp'), parts along dimension 0
There are 4 independent parts. The reference program is written for one: setup_inputs(seed, part) draws one part's arguments, and reference() takes and returns one part's arrays. A program takes and returns all parts, laid end to end along the dimension named above; an argument that names none is the same for every part.
All inputs are finite; a program needn't handle non-finite values.
Results may differ from the reference program's by a relative error of at most 0.0245.
Values are sent between devices in bfloat16 or wider.
A program may use at most 768 MiB of HBM per device.

```python
import jax
import jax.numpy as jnp
from jax import lax

SEQUENCES = 16
TOKENS = 2048
D = 512
HEADS = 8
KV_HEADS = 4
HEAD = 128
FF = 1536
LAYERS = 2
THETA = 10000
NAMES = ("wq", "wk", "wv", "wo", "w_gate", "w_up", "w_down")
SHAPES = {
    "wq": (LAYERS, D, HEADS * HEAD),
    "wk": (LAYERS, D, KV_HEADS * HEAD),
    "wv": (LAYERS, D, KV_HEADS * HEAD),
    "wo": (LAYERS, HEADS * HEAD, D),
    "w_gate": (LAYERS, D, FF),
    "w_up": (LAYERS, D, FF),
    "w_down": (LAYERS, FF, D),
}


def bump(key, n, height):
    away = (jnp.arange(n, dtype=jnp.int32) - jax.random.randint(key, (), 0, n, jnp.int32)) % n
    return jnp.where(away < n // 8, height, 1.0)


def together(key, own, strength):
    shared = jax.random.normal(key, own.shape[1:], jnp.float32)
    return (own + strength * shared) * lax.rsqrt(1 + strength * strength)


def setup_inputs(seed: int = 0, part: int = 0) -> dict:
    kx, kdy, ka, kb, kz, kf, kh, kl, *keys = jax.random.split(jax.random.key(seed), 8 + 3 * len(NAMES))
    kx, kdy, ka, kb = (jax.random.fold_in(k, part) for k in (kx, kdy, ka, kb))
    kw, km, kv = (keys[i::3] for i in range(3))
    shape = (SEQUENCES, TOKENS, D)
    much_x, much_dy = jax.random.uniform(kz, (2,), jnp.float32, 0.0, 1.0)
    loud = 2.0 ** jax.random.uniform(jax.random.fold_in(kz, 1), (), jnp.float32, -1.0, 2.0)
    layers = 2.0 ** jax.random.uniform(kl, (LAYERS, 1, 1), jnp.float32, -1.0, 1.0)
    times = {"wq": 1.0, "wk": 1.0, "wv": 2.0, "wo": layers, "w_gate": 1.0, "w_up": bump(kh, FF, 4.0), "w_down": layers}
    x = together(ka, jax.random.normal(kx, shape, jnp.float32), much_x) * bump(kf, D, 4.0)
    dy = together(kb, jax.random.normal(kdy, shape, jnp.float32), much_dy)
    drawn = {"x": x.astype(jnp.bfloat16), "dy": (loud * dy * (SEQUENCES * TOKENS) ** -0.5).astype(jnp.bfloat16)}
    for key, name in zip(kw, NAMES, strict=True):
        drawn[name] = (jax.random.normal(key, SHAPES[name], jnp.float32) * SHAPES[name][1] ** -0.5 * times[name]).astype(jnp.bfloat16)
    for key, name in zip(km, NAMES, strict=True):
        drawn[f"m_{name}"] = 0.1 * jax.random.normal(key, SHAPES[name], jnp.float32)
    for key, name in zip(kv, NAMES, strict=True):
        drawn[f"v_{name}"] = loud * loud * jax.random.uniform(key, SHAPES[name], jnp.float32, 0.2, 0.6)
    return drawn


def matmul(a, w):
    return jnp.dot(a, w, preferred_element_type=jnp.float32).astype(jnp.bfloat16)


def normed(h):
    wide = h.astype(jnp.float32)
    scale = lax.rsqrt(jnp.mean(wide**2, -1, keepdims=True) + 1e-6)
    return (wide * scale).astype(jnp.bfloat16)


def turned(t, theta):
    half = t.shape[-1] // 2
    angle = jnp.arange(t.shape[0], dtype=jnp.float32)[:, None] * theta ** (-jnp.arange(half, dtype=jnp.float32) / half)
    cos, sin = jnp.cos(angle)[:, None], jnp.sin(angle)[:, None]
    a, b = t[..., :half].astype(jnp.float32), t[..., half:].astype(jnp.float32)
    return jnp.concatenate([a * cos - b * sin, b * cos + a * sin], -1).astype(jnp.bfloat16)


def seen_by(q, k, v):
    tokens, kv = q.shape[0], k.shape[1]
    q = q.reshape(tokens, kv, -1, q.shape[-1])
    scores = jnp.einsum("tgsd,ugd->gstu", q.astype(jnp.float32), k.astype(jnp.float32)) * q.shape[-1] ** -0.5
    place = jnp.arange(tokens)
    weights = jax.nn.softmax(jnp.where(place[:, None] >= place, scores, -jnp.inf), -1).astype(jnp.bfloat16)
    return jnp.einsum("gstu,ugd->tgsd", weights.astype(jnp.float32), v.astype(jnp.float32)).astype(jnp.bfloat16).reshape(tokens, -1)


def layer(h, w):
    a = normed(h)
    q, k = (turned(matmul(a, w[name]).reshape(h.shape[0], -1, HEAD), THETA) for name in ("wq", "wk"))
    h = h + matmul(seen_by(q, k, matmul(a, w["wv"]).reshape(h.shape[0], -1, HEAD)), w["wo"])
    b = normed(h)
    gate = jnp.dot(b, w["w_gate"], preferred_element_type=jnp.float32)
    up = jnp.dot(b, w["w_up"], preferred_element_type=jnp.float32)
    return h + matmul((jax.nn.silu(gate) * up).astype(jnp.bfloat16), w["w_down"])


def adamw(w, m, v, g):
    m = 0.9 * m + 0.1 * g
    v = 0.95 * v + 0.05 * g * g
    step = m * lax.rsqrt(v + 1e-8) + 0.1 * w
    return (w - 0.02 * step).astype(jnp.bfloat16), m, v


def stack(weights, h):
    return lax.scan(lambda h, w: (layer(h, w), None), h, weights)[0]


def reference(x, dy, wq, wk, wv, wo, w_gate, w_up, w_down, m_wq, m_wk, m_wv, m_wo, m_w_gate, m_w_up, m_w_down, v_wq, v_wk, v_wv, v_wo, v_w_gate, v_w_up, v_w_down):
    weights = dict(zip(NAMES, (wq, wk, wv, wo, w_gate, w_up, w_down), strict=True))

    def take(so_far, sequence):
        h, by_y = sequence
        _, back = jax.vjp(stack, weights, h)
        by_weights, by_h = back(by_y)
        return jax.tree.map(lambda total, term: total + term.astype(jnp.float32), so_far, by_weights), by_h

    none_yet = {name: jnp.zeros(w.shape, jnp.float32) for name, w in weights.items()}
    by_weights, by_x = lax.scan(take, none_yet, (x, dy))
    gradients = [by_weights[name].astype(jnp.bfloat16).astype(jnp.float32) for name in NAMES]
    first = (m_wq, m_wk, m_wv, m_wo, m_w_gate, m_w_up, m_w_down)
    second = (v_wq, v_wk, v_wv, v_wo, v_w_gate, v_w_up, v_w_down)
    new = [adamw(weights[name].astype(jnp.float32), m, v, g) for name, m, v, g in zip(NAMES, first, second, gradients, strict=True)]
    return tuple(one[which] for which in range(3) for one in new)
```

```python
import functools

import jax
import jax.numpy as jnp
import numpy as np
from jax import lax
from jax.experimental import pallas as pl
from jax.experimental.pallas import tpu as pltpu
from jax.sharding import PartitionSpec as P

HEAD = 128
THETA = 10000
NEG = -1e30
HIDDEN = 2 * NEG
LOG2E = 1.4426950408889634
SCALE = HEAD**-0.5
E = SCALE * LOG2E
EPS = 1e-6
CHUNKS = 2


def _dot(a, b, ca=1, cb=0):
    return lax.dot_general(a, b, (((ca,), (cb,)), ((), ())), preferred_element_type=jnp.float32)


def _rows_dot(a, b):
    return _dot(a, b, 1, 1)


def _cols_dot(a, b):
    return _dot(a, b, 0, 0)


def _params(dims, **more):
    return pltpu.CompilerParams(dimension_semantics=("arbitrary",) * dims or None, vmem_limit_bytes=62 * 2**20, **more)


def _talks(number):
    return dict(collective_id=number, has_side_effects=True)


def _norm(h):
    wide = h.astype(jnp.float32)
    scale = lax.rsqrt(jnp.mean(wide * wide, -1, keepdims=True) + EPS)
    return (wide * scale).astype(jnp.bfloat16), wide, scale


def _norm_back(by, wide, scale):
    inner = jnp.mean(by * wide, -1, keepdims=True)
    return by * scale - wide * (scale * scale * scale * inner)


def _turn(x, cos, sin):
    return [x[:, n : n + HEAD] * cos + pltpu.roll(x[:, n : n + HEAD], HEAD // 2, 1) * sin for n in range(0, x.shape[1], HEAD)]


def _tall(ref, at, rows):
    n, _, d = ref.shape
    return ref[:, at : at + rows // n, :].reshape(rows, d)


def _panel(ref, col, at=0):
    n, _, d = ref.shape
    return _tall(ref, at + col // d * (d // n), d)


def _rows(rows, *cols):
    return [pl.BlockSpec((rows, c), lambda i: (i, 0)) for c in cols]


def _whole(shape):
    return pl.BlockSpec(shape, lambda *_: (0,) * len(shape), pipeline_mode=pl.Buffered(1))


MESH = pl.DeviceIdType.MESH


def _places(n):
    me = lax.axis_index("dp")
    chips = n // 2
    chip, core = lax.div(me, 2), lax.rem(me, 2)
    return chip, core, chips, lambda off, c: 2 * lax.rem(chip + off + 2 * chips, chips) + c


def _greet(n):
    _, core, _, at = _places(n)
    barrier = pltpu.get_barrier_semaphore()
    for other in (at(1, core), at(-1, core), at(0, 1 - core)):
        pl.semaphore_signal(barrier, inc=1, device_id={"dp": other}, device_id_type=MESH)
    pl.semaphore_wait(barrier, 3)


def _ways(chips, chunk):
    far = chips // 2
    return ((1, far), (-1, chips - 1 - far)) if chunk % 2 == 0 else ((1, chips - 1 - far), (-1, far))


def _lane(way):
    return (1 - way) // 2


def _send(src, dst, send, recv, to):
    return pltpu.make_async_remote_copy(src_ref=src, dst_ref=dst, send_sem=send, recv_sem=recv, device_id={"dp": to}, device_id_type=MESH)


def gather_sems(n, chunks):
    dma = pltpu.SemaphoreType.DMA
    return [dma((2, chunks, n // 4)), dma((2, chunks, n // 4)), dma((chunks, n // 2)), dma((chunks, n // 2)), dma((chunks,))]


def gather_events(chunks, sems):
    ring_out, ring_in, twin_out, twin_in, held = sems
    n = chunks[0][0].shape[0]
    _, core, chips, at = _places(n)
    twin = at(0, 1 - core)

    def part(j, i):
        ref, lo, rows, _ = chunks[j]
        return ref.at[i, pl.ds(lo, rows), :]

    def sources(j):
        ref, lo, _, given = chunks[j]
        return [(source, ref.at[at(0, core), pl.ds(row, source.shape[0]), :]) for source, row in given]

    def hop(way, j, h):
        here = part(j, at(-way * h, core))
        return _send(here, here, ring_out.at[_lane(way), j, h], ring_in.at[_lane(way), j, h], at(way, core))

    def slot(way, j, h):
        return h if way > 0 or h == 0 else _ways(chips, j)[0][1] + h

    def across(way, j, h, c):
        here = part(j, at(-way * h, c))
        return _send(here, here, twin_out.at[j, slot(way, j, h)], twin_in.at[j, slot(way, j, h)], twin)

    def begin():
        for j in range(len(chunks)):
            for way, _ in _ways(chips, j):
                for source, target in sources(j):
                    _send(source, target, ring_out.at[_lane(way), j, 0], ring_in.at[_lane(way), j, 0], at(way, core)).start()
        for j in range(len(chunks)):
            for source, target in sources(j):
                _send(source, target, twin_out.at[j, 0], twin_in.at[j, 0], twin).start()
                pltpu.make_async_copy(source, target, held.at[j]).start()

    def arrive(j, h):
        for way, far in _ways(chips, j):
            if h <= far:
                hop(way, j, h - 1).wait_recv()
                if h < far:
                    hop(way, j, h).start()
                across(way, j, h, core).start()

    def finish():
        for j in range(len(chunks)):
            mine = part(j, at(0, core))
            pltpu.make_async_copy(mine, mine, held.at[j]).wait()
            for way, far in _ways(chips, j):
                for h in range(0 if way > 0 else 1, far + 1):
                    across(way, j, h, core).wait_send()
                    across(way, j, h, 1 - core).wait_recv()
                for h in range(far):
                    hop(way, j, h).wait_send()

    return [begin, *[functools.partial(arrive, j, h) for h in range(1, n // 4 + 1) for j in range(len(chunks))], finish]


def scatter_scratch(n, rows, d, staged=True):
    far, chips = n // 4, n // 2
    block, hops = pltpu.VMEM((chips, rows, d), jnp.bfloat16), pltpu.VMEM((2, CHUNKS, far, rows // CHUNKS, d), jnp.bfloat16)
    ring, twin = pltpu.SemaphoreType.DMA((2, CHUNKS, far)), pltpu.SemaphoreType.DMA((chips,))
    return [block, hops, hops, ring, ring, twin, twin] + [block, twin] * staged


def scatter_events(term_ref, sum_ref, scratch):
    chunks = CHUNKS
    from_twin, going, coming, ring_out, ring_in, twin_out, twin_in, *stage = scratch
    mine, held = stage or (None, None)
    n, rows, _ = term_ref.shape
    chip, core, chips, at = _places(n)
    twin = at(0, 1 - core)
    size = rows // chunks
    across = lambda i: _send(term_ref.at[at(i, 1 - core)], from_twin.at[i], twin_out.at[i], twin_in.at[i], twin)
    fetch = lambda i: pltpu.make_async_copy(term_ref.at[at(i, core)], mine.at[i], held.at[i])
    hop = lambda way, j, h: _send(going.at[_lane(way), j, h], coming.at[_lane(way), j, h], ring_out.at[_lane(way), j, h], ring_in.at[_lane(way), j, h], at(way, core))
    order = [i for k in range(chips // 2, -1, -1) for i in ([k, chips - k] if 0 < k < chips / 2 else [k])]

    def own(off, j):
        i = off % chips
        if j == 0:
            if stage:
                fetch(i).wait()
            across(i).wait_recv()
        rows_j = pl.ds(j * size, size)
        term = mine[i, rows_j, :] if stage else term_ref[at(i, core), rows_j, :]
        return term.astype(jnp.float32) + from_twin[i, rows_j, :].astype(jnp.float32)

    def begin():
        for i in order:
            if stage:
                fetch(i).start()
            across(i).start()

    def forward(j, k):
        for way, far in _ways(chips, j):
            if far >= k:
                h = far - k
                total = own(way * k, j)
                if h:
                    hop(way, j, h - 1).wait_recv()
                    total = total + coming[_lane(way), j, h - 1].astype(jnp.float32)
                going[_lane(way), j, h] = total.astype(jnp.bfloat16)
                hop(way, j, h).start()

    def finish(j):
        total = own(0, j)
        for way, far in _ways(chips, j):
            hop(way, j, far - 1).wait_recv()
            total = total + coming[_lane(way), j, far - 1].astype(jnp.float32)
        sum_ref[pl.ds(j * size, size), :] = total.astype(sum_ref.dtype)

    def close():
        for i in order:
            across(i).wait_send()
        for j in range(chunks):
            for way, far in _ways(chips, j):
                for h in range(far):
                    hop(way, j, h).wait_send()

    return [begin, *[functools.partial(forward, j, k) for k in range(n // 4, 0, -1) for j in range(chunks)],
            *[functools.partial(finish, j) for j in range(chunks)], close]


def _hosted(events, at, now, pace=1):
    def due():
        for point in sorted(set(at)):
            these = [event for event, when in zip(events, at, strict=True) if when == point]
            pl.when(now == point)(functools.partial(_all, these))

    if events:
        pl.when(lax.rem(now, pace) == 0)(due) if pace > 1 else due()


def _all(events):
    for event in events:
        event()


def _spread(count, last, pace, first=1):
    return [0] + [pace * (first + i * (last // pace - first) // (count - 2)) for i in range(count - 1)]


def _parts(refs, layer, d):
    out, at = [], 0
    for ref in refs:
        for c in range(0, ref.shape[2], d):
            out.append((ref.at[layer, :, pl.ds(c, d)], at))
            at += ref.shape[1]
    return out, at


def _cut(all_ref, refs, layer, groups):
    d, chunks, at = all_ref.shape[2], [], 0
    for group in groups:
        parts, rows = _parts([refs[name] for name in group], layer, d)
        chunks.append((all_ref, at, rows, [(source, at + row) for source, row in parts]))
        at += rows
    return chunks


def _held(w, names, d):
    return sum(w[name].shape[1] * (w[name].shape[2] // d) for name in names)


NAMES = ("wq", "wk", "wv", "wo", "w_gate", "w_up", "w_down")
FIRST = (("wq",), ("wk", "wv"))
TALL = (("wo",), ("w_down",))
WIDE = (("w_gate",), ("w_up",))


def _names(groups):
    return [name for group in groups for name in group]


def _angles(freq, out_refs):
    t = out_refs[0].shape[0]
    fine = HEAD // 4
    count = lambda n: lax.broadcasted_iota(jnp.int32, (n, HEAD), 0).astype(jnp.float32)
    a, b = count(t // fine) * fine * freq, count(fine) * freq
    ca, sa, cb, sb = (x.reshape(-1, 1, HEAD) if x.shape[0] > fine else x[None] for x in (jnp.cos(a), jnp.sin(a), jnp.cos(b), jnp.sin(b)))
    sign = jnp.where(lax.broadcasted_iota(jnp.int32, (1, 1, HEAD), 2) < HEAD // 2, -1.0, 1.0)
    out_refs[0][...] = (ca * cb - sa * sb).reshape(t, HEAD)
    out_refs[1][...] = ((sa * cb + ca * sb) * sign).reshape(t, HEAD)


def _project(h, w_ref, cos, sin, outs, rows):
    a, _, _ = _norm(h)
    d, at = h.shape[1], 0
    for out, turn in zip(outs, (True, True, False), strict=True):
        for n in range(0, out.shape[1], d):
            x = _dot(a, _panel(w_ref, at)).astype(jnp.bfloat16)
            at += d
            if turn:
                for i, part in enumerate(_turn(x.astype(jnp.float32), cos, sin)):
                    out[rows, n + i * HEAD : n + (i + 1) * HEAD] = part.astype(jnp.bfloat16)
            else:
                out[rows, n : n + d] = x


def _attend(q_ref, k_ref, v_ref, o_ref, lse_ref, top_s, mix_s, host, bq, bk):
    t = q_ref.shape[0]
    kv = k_ref.shape[1] // HEAD
    g = q_ref.shape[1] // k_ref.shape[1]
    pieces = [(i, n) for i in range(kv) for n in range(g)]
    col = lambda i, n: slice((i * g + n) * HEAD, (i * g + n + 1) * HEAD)
    key = lambda i: slice(i * HEAD, (i + 1) * HEAD)
    ones = jnp.ones((8, bk), jnp.bfloat16)
    per = bq // bk

    def queries(iq, _):
        gap = lax.broadcasted_iota(jnp.int32, (bk, bq), 1) - lax.broadcasted_iota(jnp.int32, (bk, bq), 0)
        rows = pl.ds(pl.multiple_of(iq * bq, bq), bq)
        top_s[...] = jnp.full_like(top_s, NEG)
        mix_s[...] = jnp.zeros_like(mix_s)

        def block(j, level):
            host(lax.div(iq * (iq + 1) * per, 2) + j)
            here = pl.ds(pl.multiple_of(j * bk, bk), bk)
            scores = [_rows_dot(k_ref[here, key(i)], q_ref[rows, col(i, n)]) for i, n in pieces]
            weights, keeps = [], []
            for p, s in enumerate(scores):
                if level is not None:
                    s = jnp.where(gap >= level, s, HIDDEN)
                old = top_s[p : p + 1, :]
                top = jnp.maximum(old, s.max(axis=0, keepdims=True))
                top_s[p : p + 1, :] = top
                weights.append(jnp.exp2((s - top) * E).astype(jnp.bfloat16))
                keeps.append(jnp.exp2((old - top) * E))
            values = [jnp.concatenate([v_ref[here, key(i)].T, ones], axis=0) for i in range(kv)]
            for p, (i, n) in enumerate(pieces):
                mix_s[p] = mix_s[p] * keeps[p] + _dot(values[i], weights[p])

        lax.fori_loop(0, iq * per, lambda j, _: block(j, None), None)
        for n in range(per):
            block(iq * per + n, n * bk)
        for p, (i, n) in enumerate(pieces):
            total = mix_s[p, HEAD : HEAD + 1, :]
            o_ref[rows, col(i, n)] = (mix_s[p, :HEAD, :] * (1 / total)).T.astype(o_ref.dtype)
            lse_ref[p : p + 1, rows] = top_s[p : p + 1, :] * SCALE + jnp.log(total)

    lax.fori_loop(0, t // bq, queries, None)


def _into(no, tall_ref):
    n = tall_ref.shape[0]
    return _tall(tall_ref, 0, no), _tall(tall_ref, no // n, n * tall_ref.shape[1] - no)


def _add(h, x):
    return (h.astype(jnp.float32) + x.astype(jnp.bfloat16).astype(jnp.float32)).astype(jnp.bfloat16)


def _rest(h, o, tall_ref, wide_ref):
    d = h.shape[1]
    wo, wd = _into(o.shape[1], tall_ref)
    h2 = _add(h, _dot(o, wo))
    b, _, _ = _norm(h2)
    ff = wd.shape[0]
    down = None
    for n in range(0, ff, d):
        gate, up = _dot(b, _panel(wide_ref, n)), _dot(b, _panel(wide_ref, ff + n))
        act = (gate * jax.nn.sigmoid(gate) * up).astype(jnp.bfloat16)
        more = _dot(act, wd[n : n + d, :])
        down = more if down is None else down + more
    return h2, _add(h2, down)


def _plan(chunks, begin, starts):
    at, count = [begin], 0.0
    for hop in range(4):
        for size in chunks:
            count += size
            due = starts[begin] + 4 + count + 1.5 * hop
            at.append(min(len(starts) - 1, sum(s < due for s in starts)))
    return at + [at[-1]]


def _forward(*refs, layers, count, bt, bq, bk):
    (x_ref, freq_ref), shards, refs = refs[:2], dict(zip(NAMES, refs[2 : 2 + len(NAMES)], strict=True)), refs[2 + len(NAMES) :]
    kept, outs, refs = [], refs[: count], refs[count:]
    h_s, h2_s, q_s, k_s, v_s, o_s, cos_s, sin_s, lse_s, top_s, mix_s, *refs = refs
    first_s, tall_s, wide_s = (refs[i * layers : (i + 1) * layers] for i in range(3))
    arrive, done, *sems = refs[3 * layers :]
    outs, (cos_ref, sin_ref) = outs[:-2], outs[-2:]
    t, d = h_s.shape
    blocks, pairs = t // bt, (t // bq) * (t // bq + 1) // 2 * (bq // bk)

    starts, phase, now = [], {}, 0.0
    for i in range(layers):
        for name, number, us in (("pre", blocks, 2.0), ("attend", pairs, 3.1), ("rest", blocks, 4.2))[: 3 if i < layers - 1 else 2]:
            phase[name, i] = len(starts)
            for _ in range(number):
                starts.append(now)
                now += us
    todo = {}

    def put(tick, event):
        todo.setdefault(tick, []).append(event)

    def host(name, i):
        base = phase[name, i]
        end = min([b for b in phase.values() if b > base], default=len(starts))
        mine = [(tick - base, todo[tick]) for tick in sorted(todo) if base <= tick < end]

        def run(now):
            for tick, events in mine:
                pl.when(now == tick)(functools.partial(_all, events))

        return run

    engines, each = [], len(sems) // (2 * layers)
    need = gather_events(_cut(first_s[0], shards, 0, FIRST), sems[:each])
    size = lambda ref, names: [sum(shards[name].shape[1] * (shards[name].shape[2] // d) for name in group) * 0.02 for group in names]
    after = lambda i: gather_events(_cut(tall_s[i], shards, i, TALL) + _cut(wide_s[i], shards, i, WIDE), sems[each * (2 * i + 1) : each * (2 * i + 2)])
    writes = []

    def write(source, target):
        copy = pltpu.make_async_copy(source, target, done.at[len(writes)])
        writes.append(copy)
        return copy

    names = {}
    at = 0
    for i in range(layers):
        take = ["q", "k", "v", "o", "lse", "tall", "wide"] + ["first"] * (i > 0) + ["h2", "h"] * (i < layers - 1)
        names[i] = dict(zip(take, outs[at : at + len(take)], strict=True))
        at += len(take)
    for i in range(layers):
        begin = 0 if i == 0 else phase["pre", i] - 1
        events = after(i)
        plan = _plan(size(None, TALL + WIDE), begin, starts)
        last = phase["attend", i] + pairs - 1
        for event, tick in zip(events[:-1], plan[:-1], strict=True):
            put(min(tick, last), event)
        names[i]["last"] = events[-1]
        if i > 0:
            events = gather_events(_cut(first_s[i], shards, i, FIRST), sems[each * 2 * i : each * (2 * i + 1)])
            plan = _plan(size(None, FIRST), phase["rest", i - 1] - 5, starts)
            last = phase["pre", i] - 1
            for event, tick in zip(events[:-1], plan[:-1], strict=True):
                put(min(tick, last), event)
            names[i]["soon"] = events[-1]

    def each_block(name, i, work):
        run = host(name, i)

        def body(step, _):
            run(step)
            work(pl.ds(pl.multiple_of(step * bt, bt), bt))

        lax.fori_loop(0, blocks, body, None)

    _greet(first_s[0].shape[0])
    need[0]()
    take = pltpu.make_async_copy(x_ref, h_s, arrive.at[0])
    take.start()
    _angles(freq_ref[...], (cos_s, sin_s))
    _all(need[1:])
    take.wait()
    starting = [write(cos_s, cos_ref), write(sin_s, sin_ref)]
    _all([copy.start for copy in starting])
    pending = []
    for i in range(layers):
        to = names[i]
        _all([copy.wait for copy in pending])
        each_block("pre", i, lambda rows, i=i: _project(h_s[rows, :], first_s[i], cos_s[rows, :], sin_s[rows, :], (q_s, k_s, v_s), rows))
        pending = [write(source, to[name]) for source, name in ((q_s, "q"), (k_s, "k"), (v_s, "v"))]
        _all([copy.start for copy in pending])
        _attend(q_s, k_s, v_s, o_s, lse_s, top_s, mix_s, host("attend", i), bq, bk)
        to["last"]()
        more = [write(source, to[name]) for source, name in ((o_s, "o"), (lse_s, "lse"), (tall_s[i], "tall"), (wide_s[i], "wide"))]
        if i > 0:
            more.append(write(first_s[i], to["first"]))
        _all([copy.start for copy in more])
        pending += more
        if i < layers - 1:

            def rest(rows, i=i):
                h2, h3 = _rest(h_s[rows, :], o_s[rows, :], tall_s[i], wide_s[i])
                h2_s[rows, :] = h2
                h_s[rows, :] = h3

            each_block("rest", i, rest)
            names[i + 1]["soon"]()
            more = [write(h2_s, to["h2"]), write(h_s, to["h"])]
            _all([copy.start for copy in more])
            pending += more
    _all([copy.wait for copy in starting + pending])


def forward(x, w, n, number, bt=512, bq=512, bk=512):
    t, d = x.shape
    layers = w["wq"].shape[0]
    nq, nk = w["wq"].shape[2], w["wk"].shape[2]
    heads = nq // HEAD
    half = HEAD // 2
    freq = np.float32(THETA) ** (-np.arange(half, dtype=np.float32) / half)
    first, tall, wide = ((n, _held(w, _names(groups), d), d) for groups in (FIRST, TALL, WIDE))
    low, wide_type = jnp.bfloat16, jnp.float32
    take, shapes = [], []
    for i in range(layers):
        one = {"q": (t, nq), "k": (t, nk), "v": (t, nk), "o": (t, nq), "lse": (heads, t), "tall": tall, "wide": wide}
        if i > 0:
            one["first"] = first
        if i < layers - 1:
            one |= {"h2": (t, d), "h": (t, d)}
        take.append(list(one))
        shapes += [jax.ShapeDtypeStruct(shape, wide_type if name == "lse" else low) for name, shape in one.items()]
    shapes += [jax.ShapeDtypeStruct((t, HEAD), wide_type)] * 2
    anywhere = pl.BlockSpec(memory_space=pl.ANY)
    sems = []
    for _ in range(layers):
        sems += gather_sems(n, len(FIRST)) + gather_sems(n, len(TALL + WIDE))
    ff = w["w_gate"].shape[2]
    out = pl.pallas_call(
        functools.partial(_forward, layers=layers, count=len(shapes), bt=bt, bq=bq, bk=bk),
        in_specs=[anywhere, pl.BlockSpec(memory_space=pltpu.VMEM)] + [anywhere] * len(NAMES),
        out_specs=[anywhere] * len(shapes),
        out_shape=shapes,
        scratch_shapes=[*[pltpu.VMEM((t, c), low) for c in (d, d, nq, nk, nk, nq)], *[pltpu.VMEM((t, HEAD), wide_type)] * 2, pltpu.VMEM((heads, t), wide_type),
                        pltpu.VMEM((heads, bq), wide_type), pltpu.VMEM((heads, HEAD + 8, bq), wide_type), *[pltpu.VMEM(first, low)] * layers,
                        *[pltpu.VMEM(tall, low)] * layers, *[pltpu.VMEM(wide, low)] * layers, pltpu.SemaphoreType.DMA((1,)), pltpu.SemaphoreType.DMA((len(shapes),)), *sems],
        compiler_params=_params(0, **_talks(number)),
        name="forward",
        cost_estimate=pl.CostEstimate(flops=2 * t * layers * (d * (2 * nq + 2 * nk + 3 * ff) + t * nq), transcendentals=t * t * heads, bytes_accessed=t * nq * 20),
    )(x, jnp.asarray(np.concatenate([freq, freq])[None]), *[w[name] for name in NAMES])
    each = []
    for names in take:
        each.append(dict(zip(names, out[: len(names)], strict=True)))
        out = out[len(names) :]
    return each, out[0], out[1]


def _attend_back(*refs, bq, bt, first):
    (q_ref, k_ref, v_ref, do_ref, o_ref, lse_ref, term_ref, h_ref, cos_ref, sin_ref), refs = refs[:10], refs[10:]
    if first:
        (sum_ref, own_ref, g_ref), refs = refs[:3], refs[3:]
    else:
        (w_ref, by_ref, sum_ref, by0_ref, g_ref), refs = refs[:5], refs[5:]
    (dq_s, all_s, dk_s, dv_s, g_s), scratch = refs[:5], refs[5:]
    step, d = pl.program_id(0), h_ref.shape[1]
    t, nk = k_ref.shape
    nq, blocks = q_ref.shape[1], t // bq
    kv, g, bk = nk // HEAD, nq // nk, bq
    staged = len(scatter_scratch(*term_ref.shape))
    events = scatter_events(term_ref, sum_ref, scratch[:staged])
    points = _spread(len(events) - 1, blocks * (blocks + 1) // 2 - 1, 3)
    pieces = [(i, n) for i in range(kv) for n in range(g)]
    col = lambda i, n: slice((i * g + n) * HEAD, (i * g + n + 1) * HEAD)
    key = lambda i: slice(i * HEAD, (i + 1) * HEAD)

    @pl.when(step == 0)
    def _():
        _greet(term_ref.shape[0])
        for s in (dk_s, dv_s, g_s):
            s[...] = jnp.zeros_like(s)

    @pl.when(step < blocks)
    def _():
        rows = pl.ds(pl.multiple_of(step * bq, bq), bq)
        dq_s[...] = jnp.zeros_like(dq_s)
        lses = [lse_ref[p : p + 1, rows] * LOG2E for p in range(len(pieces))]
        deltas = [(do_ref[:, col(i, n)].astype(jnp.float32) * o_ref[:, col(i, n)].astype(jnp.float32)).T.sum(axis=0, keepdims=True) for i, n in pieces]
        gap = lax.broadcasted_iota(jnp.int32, (bk, bq), 1) - lax.broadcasted_iota(jnp.int32, (bk, bq), 0)

        def block(j, masked):
            _hosted(events[:-1], points, lax.div(step * (step + 1), 2) + j, 3)
            here = pl.ds(pl.multiple_of(j * bk, bk), bk)
            scores = [_rows_dot(k_ref[here, key(i)], q_ref[:, col(i, n)]) for i, n in pieces]
            dps = [_rows_dot(v_ref[here, key(i)], do_ref[:, col(i, n)]) for i, n in pieces]
            for m, (i, n) in enumerate(pieces):
                p = jnp.exp2(scores[m] * E - lses[m])
                if masked:
                    p = jnp.where(gap >= 0, p, 0.0)
                ds = (p * (dps[m] - deltas[m])).astype(jnp.bfloat16)
                dv_s[here, key(i)] += _dot(p.astype(jnp.bfloat16), do_ref[:, col(i, n)])
                dk_s[here, key(i)] += _dot(ds, q_ref[:, col(i, n)])
                dq_s[m] += _dot(k_ref[here, key(i)].T, ds)

        lax.fori_loop(0, step, lambda j, _: block(j, False), None)
        block(step, True)
        for m, (i, n) in enumerate(pieces):
            all_s[rows, col(i, n)] = (dq_s[m] * SCALE).T.astype(jnp.bfloat16)

    @pl.when(step >= blocks)
    def _():
        rows = pl.ds(pl.multiple_of((step - blocks) * bt, bt), bt)
        a, wide, scale = _norm(h_ref[...])
        cos, sin = cos_ref[...], -sin_ref[...]
        panels = [(all_s[rows, c : c + d], True) for c in range(0, nq, d)]
        panels += [((dk_s[rows, c : c + d] * SCALE).astype(jnp.bfloat16), True) for c in range(0, nk, d)]
        panels += [(dv_s[rows, c : c + d].astype(jnp.bfloat16), False) for c in range(0, nk, d)]
        at, da = 0, None
        for x, turn in panels:
            if turn:
                x = jnp.concatenate([y.astype(jnp.bfloat16) for y in _turn(x.astype(jnp.float32), cos, sin)], axis=1)
            g_s[:, at : at + d] += _cols_dot(a, x)
            if not first:
                more = _rows_dot(x, _panel(w_ref, at))
                da = more if da is None else da + more
            at += d
        if not first:
            back = _norm_back(da.astype(jnp.bfloat16).astype(jnp.float32), wide, scale)
            by0_ref[...] = (by_ref[...].astype(jnp.float32) + back).astype(jnp.bfloat16)

    @pl.when(step == pl.num_programs(0) - 1)
    def _():
        n = g_ref.shape[0]
        per = d // n
        for i, c in enumerate(range(0, g_s.shape[1], d)):
            g_ref[:, i * per : (i + 1) * per, :] = g_s[:, c : c + d].reshape(n, per, d).astype(jnp.bfloat16)
        events[-1]()
        if first:
            _all(scatter_events(g_ref, own_ref, scratch[staged:]))


def attend_back(one, do, terms, h, cos, sin, number, by=None, bq=256, bt=512):
    q, k, v, o, lse = (one[name] for name in ("q", "k", "v", "o", "lse"))
    (t, nq), nk, d, n = q.shape, k.shape[1], h.shape[1], terms.shape[0]
    first = by is None
    cols, low, wide = nq + 2 * nk, jnp.bfloat16, jnp.float32
    blocks = t // bq
    own = (n, d // n * (cols // d), d)
    early = pl.BlockSpec((bq, nq), lambda i: (jnp.minimum(i, blocks - 1), 0))
    late = lambda c: pl.BlockSpec((bt, c), lambda i: (jnp.maximum(i - blocks, 0), 0))
    given = [q, k, v, do, o, lse, terms, h, cos, sin]
    specs = [early, _whole(k.shape), _whole(v.shape), early, early, _whole(lse.shape), pl.BlockSpec(memory_space=pl.ANY), late(d), late(HEAD), late(HEAD)]
    outs, out_specs, scratch = [terms.shape[1:]], [_whole(terms.shape[1:])], [pltpu.VMEM(own, low)] * first
    if first:
        outs.append(own[1:])
        out_specs.append(_whole(own[1:]))
    else:
        given += [one["first"], by]
        specs += [_whole(one["first"].shape), late(d)]
        outs += [(t, d), own]
        out_specs += [late(d), _whole(own)]
    return pl.pallas_call(
        functools.partial(_attend_back, bq=bq, bt=bt, first=first),
        grid=(blocks + t // bt,),
        in_specs=specs,
        out_specs=out_specs,
        out_shape=[jax.ShapeDtypeStruct(x, low) for x in outs],
        scratch_shapes=[*scratch, pltpu.VMEM((nq // HEAD, HEAD, bq), wide), pltpu.VMEM((t, nq), low), pltpu.VMEM((t, nk), wide), pltpu.VMEM((t, nk), wide),
                        pltpu.VMEM((d, cols), wide), *scatter_scratch(*terms.shape), *(scatter_scratch(*own, False) if first else [])],
        compiler_params=_params(1, **_talks(number)),
        name="attend_back",
        cost_estimate=pl.CostEstimate(flops=10 * t * t * nq + 4 * t * d * cols, transcendentals=t * t * nq // HEAD // 2, bytes_accessed=t * nq * 10),
    )(*given)


def _post_back(*refs, fresh, hosts, steps):
    (h_ref, o_ref, by_ref, tall_ref, wide_ref), refs = refs[:5], refs[5:]
    events = []
    if hosts:
        (term_ref, by2_ref, do_ref, g_ref, sum_ref, go_s, gg_s, gu_s, gd_s), scratch = refs[:9], refs[9:]
        events = scatter_events(term_ref, sum_ref, scratch)
        pl.when(pl.program_id(0) == 0)(lambda: _greet(term_ref.shape[0]))
    else:
        by2_ref, do_ref, g_ref, go_s, gg_s, gu_s, gd_s = refs
    step = pl.program_id(0)
    d = h_ref.shape[1]
    wo, wd = _into(o_ref.shape[1], tall_ref)
    ff = wd.shape[0]
    wg, wu = (lambda c: _panel(wide_ref, c)), (lambda c: _panel(wide_ref, ff + c))
    o = o_ref[...]
    h2 = h_ref[...]
    if fresh:
        h2 = _add(h2, _dot(o, wo))
    b, wide, scale = _norm(h2)
    by = by_ref[...]

    @pl.when(step == 0)
    def _():
        for s in (go_s, gg_s, gu_s, gd_s):
            s[...] = jnp.zeros_like(s)

    db, stops = None, ff // d
    points = _spread(len(events) - 1, steps * stops - 1, 1) if hosts else []
    for n in range(0, ff, d):
        _hosted(events[:-1], points, step * stops + n // d)
        at = slice(n, n + d)
        gate, up = _dot(b, wg(n)), _dot(b, wu(n))
        dact = _rows_dot(by, wd[at, :]).astype(jnp.bfloat16).astype(jnp.float32)
        sig = jax.nn.sigmoid(gate)
        silu = gate * sig
        act = (silu * up).astype(jnp.bfloat16)
        dup = (dact * silu).astype(jnp.bfloat16)
        dgate = (dact * up * (sig + silu * (1 - sig))).astype(jnp.bfloat16)
        gd_s[at, :] += _cols_dot(act, by)
        gg_s[:, at] += _cols_dot(b, dgate)
        gu_s[:, at] += _cols_dot(b, dup)
        more = _rows_dot(dgate, wg(n)) + _rows_dot(dup, wu(n))
        db = more if db is None else db + more
    by2 = (by.astype(jnp.float32) + _norm_back(db.astype(jnp.bfloat16).astype(jnp.float32), wide, scale)).astype(jnp.bfloat16)
    by2_ref[...] = by2
    do_ref[...] = _rows_dot(by2, wo).astype(jnp.bfloat16)
    go_s[...] += _cols_dot(o, by2)

    @pl.when(step == pl.num_programs(0) - 1)
    def _():
        n = g_ref.shape[0]
        at = 0
        for s in (go_s, gd_s, gg_s, gu_s):
            per = s.shape[0] // n
            for c in range(0, s.shape[1], d):
                g_ref[:, at : at + per, :] = s[:, c : c + d].reshape(n, per, d).astype(jnp.bfloat16)
                at += per

    if events:
        pl.when(step == pl.num_programs(0) - 1)(events[-1])


def post_back(h, o, by, tall, wide, fresh, terms=None, number=None, bt=512):
    t, d = h.shape
    no = o.shape[1]
    n = tall.shape[0]
    ff = n * tall.shape[1] - no
    shape = (n, tall.shape[1] + wide.shape[1], d)
    more, given, outs, scratch = {}, [], [], []
    if terms is not None:
        given, outs, scratch, more = [terms], [terms.shape[1:]], scatter_scratch(*terms.shape), _talks(number)
    return pl.pallas_call(
        functools.partial(_post_back, fresh=fresh, hosts=terms is not None, steps=t // bt),
        grid=(t // bt,),
        in_specs=[*_rows(bt, d, no, d), _whole(tall.shape), _whole(wide.shape)] + [pl.BlockSpec(memory_space=pl.ANY)] * len(given),
        out_specs=[*_rows(bt, d, no), _whole(shape), *[_whole(x) for x in outs]],
        out_shape=[jax.ShapeDtypeStruct(x, jnp.bfloat16) for x in ((t, d), (t, no), shape, *outs)],
        scratch_shapes=[pltpu.VMEM((no, d), jnp.float32), pltpu.VMEM((d, ff), jnp.float32), pltpu.VMEM((d, ff), jnp.float32), pltpu.VMEM((ff, d), jnp.float32)] + scratch,
        compiler_params=_params(1, **more),
        name="post_back",
        cost_estimate=pl.CostEstimate(flops=2 * t * d * (2 * no + 8 * ff), transcendentals=t * ff * 2, bytes_accessed=t * (3 * d + 2 * no) * 2),
    )(h, o, by, tall, wide, *given)


def _adamw(*refs, places, layers):
    count = len(places)
    kinds = (len(refs) - 6 * count) // layers
    grads, rest = refs[: kinds * layers], refs[kinds * layers :]
    threes = [rest[i : i + 3] for i in range(0, len(rest), 3)]

    def go(layer):
        for (block, at), given, new in zip(places, threes[:count], threes[count:], strict=True):
            g_ref = grads[layer * kinds + block]
            d = g_ref.shape[-1]
            _, rows, cols = given[0].shape
            for c in range(0, cols, d):
                g = g_ref[at : at + rows, :].astype(jnp.float32)
                at += rows
                w, m, v = (ref[0, :, c : c + d] for ref in given)
                w = w.astype(jnp.float32)
                m = 0.9 * m + 0.1 * g
                v = 0.95 * v + 0.05 * g * g
                step = m * lax.rsqrt(v + 1e-8) + 0.1 * w
                for ref, value in zip(new, ((w - 0.02 * step).astype(jnp.bfloat16), m, v), strict=True):
                    ref[0, :, c : c + d] = value

    for layer in range(layers):
        pl.when(pl.program_id(0) == layer)(functools.partial(go, layer))


def adamw(grads, given):
    places, flat = [], []
    for block, some in enumerate(given):
        at = 0
        for three in some:
            places.append((block, at))
            at += three[0][0].size // grads[0][0].shape[1]
            flat += three
    each = [pl.BlockSpec((1, *x.shape[1:]), lambda i: (i, 0, 0)) for x in flat]
    grads = [x for some in grads for x in some]
    size = sum(x.size for x in flat) // 3
    layers = flat[0].shape[0]
    out = pl.pallas_call(
        functools.partial(_adamw, places=places, layers=layers),
        grid=(layers,),
        in_specs=[_whole(x.shape) for x in grads] + each,
        out_specs=each,
        out_shape=[jax.ShapeDtypeStruct(x.shape, x.dtype) for x in flat],
        compiler_params=_params(1),
        name="adamw",
        cost_estimate=pl.CostEstimate(flops=15 * size, transcendentals=size, bytes_accessed=22 * size),
    )(*grads, *flat)
    return [out[i : i + 3] for i in range(0, len(out), 3)]


def solution(mesh):
    n = mesh.shape["dp"]

    def step(x, dy, *arrays):
        w, m, v = (dict(zip(NAMES, arrays[i : i + 7], strict=True)) for i in (0, 7, 14))
        layers = w["wq"].shape[0]
        h, by = x[0], dy[0]
        kept, cos, sin = forward(h, w, n, 1)
        g_first, g_after = [None] * layers, [None] * layers
        terms = ()
        for i in reversed(range(layers)):
            one = kept[i]
            h = kept[i - 1]["h"] if i else x[0]
            by, do, g, *got = post_back(one.get("h2", h), one["o"], by, one["tall"], one["wide"], "h2" not in one, *terms)
            if got:
                g_first[i + 1] = got[0]
            if i > 0:
                g_after[i], by, g = attend_back(one, do, g, h, cos, sin, 40 + i, by)
                terms = (g, 60 + i)
            else:
                g_after[i], g_first[i] = attend_back(one, do, g, h, cos, sin, 40 + i)
        order = [_names(FIRST), _names(TALL + WIDE)]
        got = adamw(list(zip(g_first, g_after, strict=True)), [[(w[name], m[name], v[name]) for name in names] for names in order])
        new = dict(zip(sum(order, []), got, strict=True))
        return tuple(new[name][which] for which in range(3) for name in NAMES)

    states, cut = P(("rep", "dp"), None, None), P(None, "dp", None)
    return jax.shard_map(
        step,
        mesh=mesh,
        in_specs=(states, states) + (cut,) * 21,
        out_specs=(P("rep", "dp", None),) * 21,
        check_vma=False,
    )
```

```python
import functools

import jax
import jax.numpy as jnp
import numpy as np
from jax import lax
from jax.experimental import pallas as pl
from jax.experimental.pallas import tpu as pltpu
from jax.sharding import PartitionSpec as P

HEAD = 128
THETA = 10000
NEG = -1e30
HIDDEN = 2 * NEG
LOG2E = 1.4426950408889634
SCALE = HEAD**-0.5
E = SCALE * LOG2E
EPS = 1e-6
CHUNKS = 2


def _dot(a, b, ca=1, cb=0):
    return lax.dot_general(a, b, (((ca,), (cb,)), ((), ())), preferred_element_type=jnp.float32)


def _rows_dot(a, b):
    return _dot(a, b, 1, 1)


def _cols_dot(a, b):
    return _dot(a, b, 0, 0)


def _params(dims, **more):
    return pltpu.CompilerParams(dimension_semantics=("arbitrary",) * dims or None, vmem_limit_bytes=2**26 - 2**16, **more)


def _talks(number):
    return dict(collective_id=number, has_side_effects=True)


def _norm(h):
    wide = h.astype(jnp.float32)
    scale = lax.rsqrt(jnp.mean(wide * wide, -1, keepdims=True) + EPS)
    return (wide * scale).astype(jnp.bfloat16), wide, scale


def _norm_back(by, wide, scale):
    inner = jnp.mean(by * wide, -1, keepdims=True)
    return by * scale - wide * (scale * scale * scale * inner)


def _turn(x, cos, sin):
    return [x[:, n : n + HEAD] * cos + pltpu.roll(x[:, n : n + HEAD], HEAD // 2, 1) * sin for n in range(0, x.shape[1], HEAD)]


def _tall(ref, at, rows):
    n, _, d = ref.shape
    return ref[:, at : at + rows // n, :].reshape(rows, d)


def _panel(ref, col, at=0):
    n, _, d = ref.shape
    return _tall(ref, at + col // d * (d // n), d)


def _whole(shape):
    return pl.BlockSpec(shape, lambda *_: (0,) * len(shape), pipeline_mode=pl.Buffered(1))


MESH = pl.DeviceIdType.MESH


def _places(n):
    me = lax.axis_index("dp")
    chips = n // 2
    chip, core = lax.div(me, 2), lax.rem(me, 2)
    return chip, core, chips, lambda off, c: 2 * lax.rem(chip + off + 2 * chips, chips) + c


def _tell(n, sem):
    _, core, _, at = _places(n)
    for other in (at(1, core), at(-1, core), at(0, 1 - core)):
        pl.semaphore_signal(sem, inc=1, device_id={"dp": other}, device_id_type=MESH)


def _told(sem):
    pl.semaphore_wait(sem, 3)


def _greet(n):
    barrier = pltpu.get_barrier_semaphore()
    _tell(n, barrier)
    _told(barrier)


def _ways(chips, chunk):
    far = chips // 2
    return ((1, far), (-1, chips - 1 - far)) if chunk % 2 == 0 else ((1, chips - 1 - far), (-1, far))


def _lane(way):
    return (1 - way) // 2


def _send(src, dst, send, recv, to):
    return pltpu.make_async_remote_copy(src_ref=src, dst_ref=dst, send_sem=send, recv_sem=recv, device_id={"dp": to}, device_id_type=MESH)


def gather_sems(n, chunks):
    dma = pltpu.SemaphoreType.DMA
    return [dma((2, chunks, n // 4)), dma((2, chunks, n // 4)), dma((chunks, n // 2)), dma((chunks, n // 2)), dma((chunks,))]


def gather_events(chunks, sems):
    ring_out, ring_in, twin_out, twin_in, held = sems
    n = chunks[0][0].shape[0]
    _, core, chips, at = _places(n)
    twin = at(0, 1 - core)

    def part(j, i):
        ref, lo, rows, _ = chunks[j]
        return ref.at[i, pl.ds(lo, rows), :]

    def sources(j):
        ref, lo, _, given = chunks[j]
        return [(source, ref.at[at(0, core), pl.ds(row, source.shape[0]), :]) for source, row in given]

    def hop(way, j, h):
        here = part(j, at(-way * h, core))
        return _send(here, here, ring_out.at[_lane(way), j, h], ring_in.at[_lane(way), j, h], at(way, core))

    def slot(way, j, h):
        return h if way > 0 or h == 0 else _ways(chips, j)[0][1] + h

    def across(way, j, h, c):
        here = part(j, at(-way * h, c))
        return _send(here, here, twin_out.at[j, slot(way, j, h)], twin_in.at[j, slot(way, j, h)], twin)

    def begin():
        for j in range(len(chunks)):
            for way, _ in _ways(chips, j):
                for source, target in sources(j):
                    _send(source, target, ring_out.at[_lane(way), j, 0], ring_in.at[_lane(way), j, 0], at(way, core)).start()
        for j in range(len(chunks)):
            for source, target in sources(j):
                _send(source, target, twin_out.at[j, 0], twin_in.at[j, 0], twin).start()
                pltpu.make_async_copy(source, target, held.at[j]).start()

    def arrive(j, h):
        for way, far in _ways(chips, j):
            if h <= far:
                hop(way, j, h - 1).wait_recv()
                if h < far:
                    hop(way, j, h).start()
                across(way, j, h, core).start()

    def finish():
        for j in range(len(chunks)):
            mine = part(j, at(0, core))
            pltpu.make_async_copy(mine, mine, held.at[j]).wait()
            for way, far in _ways(chips, j):
                for h in range(0 if way > 0 else 1, far + 1):
                    across(way, j, h, core).wait_send()
                    across(way, j, h, 1 - core).wait_recv()
                for h in range(far):
                    hop(way, j, h).wait_send()

    return [begin, *[functools.partial(arrive, j, h) for h in range(1, n // 4 + 1) for j in range(len(chunks))], finish]


def scatter_scratch(n, rows, d):
    far, chips = n // 4, n // 2
    ring, twin = pltpu.SemaphoreType.DMA((2, CHUNKS, far)), pltpu.SemaphoreType.DMA((chips,))
    return [pltpu.VMEM((chips, rows, d), jnp.bfloat16), pltpu.VMEM((2, CHUNKS, far, rows // CHUNKS, d), jnp.bfloat16), ring, ring, twin, twin]


def scatter_events(term_ref, sum_ref, scratch):
    totals, coming, ring_out, ring_in, twin_out, twin_in = scratch
    n, rows, _ = term_ref.shape
    _, core, chips, at = _places(n)
    twin = at(0, 1 - core)
    size = rows // CHUNKS
    part = lambda j: pl.ds(j * size, size)

    def across(i):
        return _send(term_ref.at[at(i, 1 - core)], totals.at[i], twin_out.at[i], twin_in.at[i], twin)

    def hop(way, j, h, far):
        target = coming.at[_lane(way), j, h]
        return _send(totals.at[way * (far - h) % chips, part(j), :], target, ring_out.at[_lane(way), j, h], ring_in.at[_lane(way), j, h], at(way, core))

    order = sorted(range(chips), key=lambda i: -min(i, chips - i))

    def own(i, j):
        if j == 0:
            across(i).wait_recv()
        return term_ref[at(i, core), part(j), :].astype(jnp.float32) + totals[i, part(j), :].astype(jnp.float32)

    def begin():
        for i in order:
            across(i).start()

    def forward(j, k):
        for way, far in _ways(chips, j):
            if far >= k:
                h, i = far - k, way * k % chips
                total = own(i, j)
                if h:
                    hop(way, j, h - 1, far).wait_recv()
                    total = total + coming[_lane(way), j, h - 1].astype(jnp.float32)
                totals[i, part(j), :] = total.astype(jnp.bfloat16)
                hop(way, j, h, far).start()

    def finish(j):
        total = own(0, j)
        for way, far in _ways(chips, j):
            hop(way, j, far - 1, far).wait_recv()
            total = total + coming[_lane(way), j, far - 1].astype(jnp.float32)
        sum_ref[part(j), :] = total.astype(sum_ref.dtype)

    def close():
        for i in order:
            across(i).wait_send()
        for j in range(CHUNKS):
            for way, far in _ways(chips, j):
                for h in range(far):
                    hop(way, j, h, far).wait_send()

    return [begin, *[functools.partial(forward, j, k) for k in range(n // 4, 0, -1) for j in range(CHUNKS)],
            *[functools.partial(finish, j) for j in range(CHUNKS)], close]


def _hosted(events, at, now, pace=1):
    def due():
        for point in sorted(set(at)):
            these = [event for event, when in zip(events, at, strict=True) if when == point]
            pl.when(now == point)(functools.partial(_all, these))

    if events:
        pl.when(lax.rem(now, pace) == 0)(due) if pace > 1 else due()


def _all(events):
    for event in events:
        event()


def _spread(count, last, pace, first=1):
    return [0] + [pace * (first + i * (last // pace - first) // (count - 2)) for i in range(count - 1)]


def _parts(refs, layer, d):
    out, at = [], 0
    for ref in refs:
        for c in range(0, ref.shape[2], d):
            out.append((ref.at[layer, :, pl.ds(c, d)], at))
            at += ref.shape[1]
    return out, at


def _cut(all_ref, refs, layer, groups):
    d, chunks, at = all_ref.shape[2], [], 0
    for group in groups:
        parts, rows = _parts([refs[name] for name in group], layer, d)
        chunks.append((all_ref, at, rows, [(source, at + row) for source, row in parts]))
        at += rows
    return chunks


def _held(w, names, d):
    return sum(w[name].shape[1] * (w[name].shape[2] // d) for name in names)


NAMES = ("wq", "wk", "wv", "wo", "w_gate", "w_up", "w_down")
FIRST = (("wq",), ("wk", "wv"))
TALL = (("wo",), ("w_down",))
WIDE = (("w_gate",), ("w_up",))


def _names(groups):
    return [name for group in groups for name in group]


def _angles(freq, out_refs):
    t = out_refs[0].shape[0]
    fine = HEAD // 4
    count = lambda n: lax.broadcasted_iota(jnp.int32, (n, HEAD), 0).astype(jnp.float32)
    a, b = count(t // fine) * fine * freq, count(fine) * freq
    ca, sa, cb, sb = (x.reshape(-1, 1, HEAD) if x.shape[0] > fine else x[None] for x in (jnp.cos(a), jnp.sin(a), jnp.cos(b), jnp.sin(b)))
    sign = jnp.where(lax.broadcasted_iota(jnp.int32, (1, 1, HEAD), 2) < HEAD // 2, -1.0, 1.0)
    out_refs[0][...] = (ca * cb - sa * sb).reshape(t, HEAD)
    out_refs[1][...] = ((sa * cb + ca * sb) * sign).reshape(t, HEAD)


def _project(h, w_ref, cos, sin, outs, rows):
    a, _, _ = _norm(h)
    d, at = h.shape[1], 0
    for out, turn in zip(outs, (True, True, False), strict=True):
        for n in range(0, out.shape[1], d):
            x = _dot(a, _panel(w_ref, at)).astype(jnp.bfloat16)
            at += d
            if turn:
                for i, part in enumerate(_turn(x.astype(jnp.float32), cos, sin)):
                    out[rows, n + i * HEAD : n + (i + 1) * HEAD] = part.astype(jnp.bfloat16)
            else:
                out[rows, n : n + d] = x


def _attend(q_ref, k_ref, v_ref, o_ref, lse_ref, top_s, mix_s, host, bq):
    t = q_ref.shape[0]
    kv = k_ref.shape[1] // HEAD
    g = q_ref.shape[1] // k_ref.shape[1]
    pieces = [(i, n) for i in range(kv) for n in range(g)]
    col = lambda i, n: slice((i * g + n) * HEAD, (i * g + n + 1) * HEAD)
    key = lambda i: slice(i * HEAD, (i + 1) * HEAD)
    bk = bq
    ones = jnp.ones((8, bk), jnp.bfloat16)

    def queries(iq, _):
        gap = lax.broadcasted_iota(jnp.int32, (bk, bq), 1) - lax.broadcasted_iota(jnp.int32, (bk, bq), 0)
        rows = pl.ds(pl.multiple_of(iq * bq, bq), bq)
        top_s[...] = jnp.full_like(top_s, NEG)
        mix_s[...] = jnp.zeros_like(mix_s)

        def block(j, masked):
            here = pl.ds(pl.multiple_of(j * bk, bk), bk)
            scores = [_rows_dot(k_ref[here, key(i)], q_ref[rows, col(i, n)]) for i, n in pieces]
            weights, keeps = [], []
            for p, s in enumerate(scores):
                if masked:
                    s = jnp.where(gap >= 0, s, HIDDEN)
                old = top_s[p : p + 1, :]
                top = jnp.maximum(old, s.max(axis=0, keepdims=True))
                top_s[p : p + 1, :] = top
                weights.append(jnp.exp2((s - top) * E).astype(jnp.bfloat16))
                keeps.append(jnp.exp2((old - top) * E))
            values = [jnp.concatenate([v_ref[here, key(i)].T, ones], axis=0) for i in range(kv)]
            for p, (i, n) in enumerate(pieces):
                mix_s[p] = mix_s[p] * keeps[p] + _dot(values[i], weights[p])

        def either(j, _):
            host(lax.div(iq * (iq + 1), 2) + j)
            pl.when(j < iq)(lambda: block(j, False))
            pl.when(j == iq)(lambda: block(j, True))

        lax.fori_loop(0, iq + 1, either, None)
        for p, (i, n) in enumerate(pieces):
            total = mix_s[p, HEAD : HEAD + 1, :]
            o_ref[rows, col(i, n)] = (mix_s[p, :HEAD, :] * (1 / total)).T.astype(o_ref.dtype)
            lse_ref[p : p + 1, rows] = top_s[p : p + 1, :] * SCALE + jnp.log(total)

    lax.fori_loop(0, t // bq, queries, None)


def _into(no, tall_ref):
    n = tall_ref.shape[0]
    return _tall(tall_ref, 0, no), _tall(tall_ref, no // n, n * tall_ref.shape[1] - no)


def _add(h, x):
    return (h.astype(jnp.float32) + x.astype(jnp.bfloat16).astype(jnp.float32)).astype(jnp.bfloat16)


def _rest(h, o, tall_ref, wide_ref):
    d = h.shape[1]
    wo, wd = _into(o.shape[1], tall_ref)
    h2 = _add(h, _dot(o, wo))
    b, _, _ = _norm(h2)
    ff = wd.shape[0]
    down = None
    for n in range(0, ff, d):
        gate, up = _dot(b, _panel(wide_ref, n)), _dot(b, _panel(wide_ref, ff + n))
        act = (gate * jax.nn.sigmoid(gate) * up).astype(jnp.bfloat16)
        more = _dot(act, wd[n : n + d, :])
        down = more if down is None else down + more
    return h2, _add(h2, down)


def _plan(chunks, begin, starts):
    at, count = [begin], 0.0
    for hop in range(4):
        for size in chunks:
            count += size
            due = starts[begin] + 4 + count + 1.5 * hop
            at.append(min(len(starts) - 1, sum(s < due for s in starts)))
    return at + [at[-1]]


SAVED = ("q", "k", "v", "o", "lse", "first", "tall", "wide", "inp", "mid")


def _forward(*refs, bt, bq):
    (x_ref, freq_ref), shards, refs = refs[:2], dict(zip(NAMES, refs[2 : 2 + len(NAMES)], strict=True)), refs[2 + len(NAMES) :]
    to, (cos_ref, sin_ref), refs = dict(zip(SAVED, refs, strict=False)), refs[len(SAVED) : len(SAVED) + 2], refs[len(SAVED) + 2 :]
    h_s, h2_s, q_s, k_s, v_s, o_s, cos_s, sin_s, lse_s, top_s, mix_s, first_s, tall_s, wide_s, arrive, done, *sems = refs
    (t, d), layers = h_s.shape, first_s.shape[0]
    blocks, pairs = t // bt, (t // bq) * (t // bq + 1) // 2
    lengths = {"pre": (blocks, 2.0), "attend": (pairs, 3.1), "rest": (blocks, 4.2)}
    base, each = {}, []
    for name, (number, us) in lengths.items():
        base[name] = len(each)
        each += [us] * number
    period = len(each)
    starts = [i // period * sum(each) + sum(each[: i % period]) for i in range(layers * period)]
    todo = {}

    def plan(events, groups, begin, last):
        count, due = 0.0, [starts[begin]]
        for hop in range(4):
            for group in groups:
                count += sum(shards[name].shape[1] * (shards[name].shape[2] // d) for name in group) * 0.02
                due.append(starts[begin] + 4 + count + 1.5 * hop)
        for event, when in zip(events[:-1], due, strict=True):
            todo.setdefault(min(last, sum(s < when for s in starts)), []).append(event)

    def host(name, layer):
        def run(now):
            for tick in sorted(todo):
                if base[name] <= tick % period < base[name] + lengths[name][0]:
                    pl.when(layer * period + base[name] + now == tick)(functools.partial(_all, todo[tick]))

        return run

    size = len(sems) // (2 * layers)
    engines = [sems[i : i + size] for i in range(0, len(sems), size)]
    firsts = [gather_events(_cut(first_s.at[i], shards, i, FIRST), engines[2 * i]) for i in range(layers)]
    afters = [gather_events(_cut(tall_s.at[i], shards, i, TALL) + _cut(wide_s.at[i], shards, i, WIDE), engines[2 * i + 1]) for i in range(layers)]
    for i in range(layers):
        at = i * period
        plan(afters[i], TALL + WIDE, max(at - 1, 0), at + base["rest"] - 1)
        if i:
            plan(firsts[i], FIRST, at - lengths["rest"][0] - 5, at - 1)

    def write(source, name, layer):
        return pltpu.make_async_copy(source, to[name].at[layer], done.at[SAVED.index(name)])

    def each_block(name, layer, work):
        run = host(name, layer)

        def body(step, _):
            run(step)
            work(pl.ds(pl.multiple_of(step * bt, bt), bt))

        lax.fori_loop(0, blocks, body, None)

    _greet(first_s.shape[1])
    firsts[0][0]()
    take = pltpu.make_async_copy(x_ref, h_s, arrive.at[0])
    take.start()
    _angles(freq_ref[...], (cos_s, sin_s))
    _all(firsts[0][1:])
    take.wait()
    turns = [pltpu.make_async_copy(cos_s, cos_ref, arrive.at[0]), pltpu.make_async_copy(sin_s, sin_ref, arrive.at[1])]
    _all([copy.start for copy in turns])
    slow = (("q", q_s), ("k", k_s), ("v", v_s), ("o", o_s), ("lse", lse_s), ("mid", h2_s), ("inp", h_s))

    def one(layer, _):
        inner = layer < layers - 1

        @pl.when(layer > 0)
        def _():
            for name, source in slow[:-1]:
                write(source, name, layer - 1).wait()

        keep = write(h_s, "inp", layer)
        keep.start()
        each_block("pre", layer, lambda rows: _project(h_s[rows, :], first_s.at[layer], cos_s[rows, :], sin_s[rows, :], (q_s, k_s, v_s), rows))
        for name, source in (*slow[:3], ("first", first_s.at[layer])):
            write(source, name, layer).start()
        _attend(q_s, k_s, v_s, o_s, lse_s, top_s, mix_s, host("attend", layer), bq)
        for i, events in enumerate(afters):
            pl.when(layer == i)(events[-1])
        for name, source in (*slow[3:5], ("tall", tall_s.at[layer]), ("wide", wide_s.at[layer])):
            write(source, name, layer).start()
        keep.wait()

        def rest(rows):
            h2, h3 = _rest(h_s[rows, :], o_s[rows, :], tall_s.at[layer], wide_s.at[layer])
            h2_s[rows, :] = h2
            h_s[rows, :] = h3

        @pl.when(inner)
        def _():
            each_block("rest", layer, rest)
            for i, events in enumerate(firsts[1:]):
                pl.when(layer == i)(events[-1])
            write(h2_s, "mid", layer).start()

        pl.when(layer == layers - 1)(lambda: write(h_s, "mid", layer).start())

    lax.fori_loop(0, layers, one, None)
    _all([copy.wait for copy in turns])
    for name, source in slow[:-1]:
        write(source, name, layers - 1).wait()
    for name, source in (("first", first_s), ("tall", tall_s), ("wide", wide_s)):
        for i in range(layers):
            write(source.at[i], name, i).wait()


def forward(x, w, n, number, bt=512, bq=512):
    t, d = x.shape
    layers, _, nq = w["wq"].shape
    nk, ff = w["wk"].shape[2], w["w_gate"].shape[2]
    heads = nq // HEAD
    half = HEAD // 2
    freq = np.float32(THETA) ** (-np.arange(half, dtype=np.float32) / half)
    first, tall, wide = ((n, _held(w, _names(groups), d), d) for groups in (FIRST, TALL, WIDE))
    low, full = jnp.bfloat16, jnp.float32
    shapes = dict(zip(SAVED, ((t, nq), (t, nk), (t, nk), (t, nq), (heads, t), first, tall, wide, (t, d), (t, d)), strict=True))
    outs = [jax.ShapeDtypeStruct((layers, *shape), full if name == "lse" else low) for name, shape in shapes.items()]
    outs += [jax.ShapeDtypeStruct((t, HEAD), full)] * 2
    anywhere = pl.BlockSpec(memory_space=pl.ANY)
    sems = []
    for _ in range(layers):
        sems += gather_sems(n, len(FIRST)) + gather_sems(n, len(TALL + WIDE))
    buffers = [((t, d), low), ((t, d), low), ((t, nq), low), ((t, nk), low), ((t, nk), low), ((t, nq), low), ((t, HEAD), full), ((t, HEAD), full), ((heads, t), full),
               ((heads, bq), full), ((heads, HEAD + 8, bq), full), ((layers, *first), low), ((layers, *tall), low), ((layers, *wide), low)]
    out = pl.pallas_call(
        functools.partial(_forward, bt=bt, bq=bq),
        in_specs=[anywhere, pl.BlockSpec(memory_space=pltpu.VMEM)] + [anywhere] * len(NAMES),
        out_specs=[anywhere] * len(outs),
        out_shape=outs,
        scratch_shapes=[*[pltpu.VMEM(*b) for b in buffers], pltpu.SemaphoreType.DMA((2,)), pltpu.SemaphoreType.DMA((len(SAVED),)), *sems],
        compiler_params=_params(0, **_talks(number)),
        name="forward",
        cost_estimate=pl.CostEstimate(flops=2 * t * layers * (d * (2 * nq + 2 * nk + 3 * ff) + t * nq), transcendentals=t * t * heads, bytes_accessed=t * nq * 20),
    )(x, jnp.asarray(np.concatenate([freq, freq])[None]), *[w[name] for name in NAMES])
    return dict(zip(SAVED, out, strict=False)), *out[len(SAVED) :]


def _zero(ref, rows):
    def body(i, _):
        ref[pl.ds(pl.multiple_of(i * HEAD, HEAD), HEAD), :] = jnp.zeros((HEAD, ref.shape[1]), ref.dtype)

    lax.fori_loop(0, rows // HEAD, body, None)


def _backward(*refs, bq, bt):
    (mid_ref, o_ref, dy_ref, tall_ref, wide_ref, q_ref, k_ref, v_ref, lse_ref, inp_ref, cos_ref, sin_ref, first_ref), refs = refs[:13], refs[13:]
    (after_ref, before_ref, by_s, do_s, last_s, h2_s, dq_s, delta_s, sum_s, terms_s, own_s, after_free, own_free), scratch = refs[:13], refs[13:]
    layers, (t, d) = pl.num_programs(0), by_s.shape
    place, step = pl.program_id(0), pl.program_id(1)
    layer = layers - 1 - place
    nq, nk = do_s.shape[1], k_ref.shape[2]
    kv, g, bk = nk // HEAD, nq // nk, bq
    tokens, queries = t // bt, t // bq
    n = terms_s.shape[0]
    tall_ref, wide_ref, first_ref, k_ref, v_ref = (ref.at[0] for ref in (tall_ref, wide_ref, first_ref, k_ref, v_ref))
    wo, wd = _into(nq, tall_ref)
    ff = wd.shape[0]
    cut = len(scratch) // 2
    events = scatter_events(terms_s, after_ref.at[0], scratch[:cut])
    earlier = scatter_events(own_s, before_ref.at[lax.rem(layer + (place > 0).astype(jnp.int32), layers)], scratch[cut:])
    pairs = queries * (queries + 1) // 2
    begin, begin_earlier = events[0], earlier[0]
    events[0] = lambda: (pl.when(place > 0)(lambda: _told(after_free)), begin())
    earlier[0] = lambda: (pl.when(place > 1)(lambda: _told(own_free)), begin_earlier())
    points = _spread(len(events) - 1, pairs - 1, 3)
    soon, then = earlier[: 2 * tokens - 1], earlier[2 * tokens - 1 : -1]
    pieces = [(i, m) for i in range(kv) for m in range(g)]
    col = lambda i, m: slice((i * g + m) * HEAD, (i * g + m + 1) * HEAD)
    key = lambda i: slice(i * HEAD, (i + 1) * HEAD)
    spans = ((0, nq), (nq, ff), (nq + ff, d * (ff // d)), (nq + 2 * ff, d * (ff // d)))

    @pl.when((place == 0) & (step == 0))
    def _():
        _greet(n)

    @pl.when(step < tokens)
    def _():
        rows = pl.ds(pl.multiple_of(step * bt, bt), bt)
        _hosted(soon, [0] + [1 + i // 2 for i in range(len(soon) - 1)], jnp.where(place > 0, step, -1))
        pl.when(step == 0)(lambda: _zero(sum_s, nq + 3 * ff))

        @pl.when(place == 0)
        def _():
            by_s[rows, :] = dy_ref[...]
            h2_s[...] = _add(mid_ref[0], _dot(o_ref[0], wo))

        @pl.when(place > 0)
        def _():
            h2_s[...] = mid_ref[0]

        o, by = o_ref[0], by_s[rows, :]
        b, wide, scale = _norm(h2_s[...])
        db = None
        for at in range(0, ff, d):
            wg, wu = _panel(wide_ref, at), _panel(wide_ref, ff + at)
            gate, up = _dot(b, wg), _dot(b, wu)
            dact = _rows_dot(by, wd[at : at + d, :]).astype(jnp.bfloat16).astype(jnp.float32)
            sig = jax.nn.sigmoid(gate)
            silu = gate * sig
            act = (silu * up).astype(jnp.bfloat16)
            dup = (dact * silu).astype(jnp.bfloat16)
            dgate = (dact * up * (sig + silu * (1 - sig))).astype(jnp.bfloat16)
            for (start, _), left, right in zip(spans[1:], (act, b, b), (by, dgate, dup), strict=True):
                sum_s[start + at : start + at + d, :] += _cols_dot(left, right)
            more = _rows_dot(dgate, wg) + _rows_dot(dup, wu)
            db = more if db is None else db + more
        by2 = (by.astype(jnp.float32) + _norm_back(db.astype(jnp.bfloat16).astype(jnp.float32), wide, scale)).astype(jnp.bfloat16)
        by_s[rows, :] = by2
        do = _rows_dot(by2, wo).astype(jnp.bfloat16)
        do_s[rows, :] = do
        sum_s[:nq, :] += _cols_dot(o, by2)
        for p, (i, m) in enumerate(pieces):
            delta_s[p : p + 1, rows] = (do[:, col(i, m)].astype(jnp.float32) * o[:, col(i, m)].astype(jnp.float32)).T.sum(axis=0, keepdims=True)

    @pl.when(step == tokens - 1)
    def _():
        at = 0
        for start, size in spans:
            panel = size if start < nq + ff else d
            for c in range(start, start + size, panel):
                terms_s[:, at : at + panel // n, :] = sum_s[c : c + panel, :].reshape(n, panel // n, d).astype(jnp.bfloat16)
                at += panel // n

    @pl.when((step >= tokens) & (step < tokens + queries))
    def _():
        iq = step - tokens
        rows = pl.ds(pl.multiple_of(iq * bq, bq), bq)
        pl.when(iq == 0)(lambda: _zero(sum_s, sum_s.shape[0]))
        dq_s[...] = jnp.zeros_like(dq_s)
        lses = [lse_ref[0, p : p + 1, rows] * LOG2E for p in range(len(pieces))]
        deltas = [delta_s[p : p + 1, rows] for p in range(len(pieces))]
        gap = lax.broadcasted_iota(jnp.int32, (bk, bq), 1) - lax.broadcasted_iota(jnp.int32, (bk, bq), 0)

        def block(j, masked):
            here, there = pl.ds(pl.multiple_of(j * bk, bk), bk), pl.ds(pl.multiple_of(t + j * bk, bk), bk)
            scores = [_rows_dot(k_ref[here, key(i)], q_ref[0, :, col(i, m)]) for i, m in pieces]
            dps = [_rows_dot(v_ref[here, key(i)], do_s[rows, col(i, m)]) for i, m in pieces]
            for x, (i, m) in enumerate(pieces):
                p = jnp.exp2(scores[x] * E - lses[x])
                if masked:
                    p = jnp.where(gap >= 0, p, 0.0)
                ds = (p * (dps[x] - deltas[x])).astype(jnp.bfloat16)
                sum_s[there, key(i)] += _dot(p.astype(jnp.bfloat16), do_s[rows, col(i, m)])
                sum_s[here, key(i)] += _dot(ds, q_ref[0, :, col(i, m)])
                dq_s[x] += _dot(k_ref[here, key(i)].T, ds)

        def either(j, _):
            now = lax.div(iq * (iq + 1), 2) + j
            _hosted(then, [3 * (1 + i) for i in range(len(then))], jnp.where(place > 0, now, -1), 3)
            _hosted(events[:-1], points, now, 3)
            pl.when(j < iq)(lambda: block(j, False))
            pl.when(j == iq)(lambda: block(j, True))

        lax.fori_loop(0, iq + 1, either, None)
        for x, (i, m) in enumerate(pieces):
            do_s[rows, col(i, m)] = (dq_s[x] * SCALE).T.astype(jnp.bfloat16)

    @pl.when((step == tokens + queries) & (place > 0))
    def _():
        earlier[-1]()
        _tell(n, own_free)

    @pl.when(step >= tokens + queries)
    def _():
        at = pl.multiple_of((step - tokens - queries) * bt, bt)
        rows = pl.ds(at, bt)
        a, wide, scale = _norm(inp_ref[0])
        cos, sin = cos_ref[...], -sin_ref[...]
        turn = lambda x: jnp.concatenate([y.astype(jnp.bfloat16) for y in _turn(x.astype(jnp.float32), cos, sin)], axis=1)
        for c in range(0, nq, d):
            do_s[rows, c : c + d] = turn(do_s[rows, c : c + d])
        h2_s[...] = turn((sum_s[rows, :] * SCALE).astype(jnp.bfloat16))
        last_s[...] = sum_s[pl.ds(t + at, bt), :].astype(jnp.bfloat16)
        panels = [do_s[rows, c : c + d] for c in range(0, nq, d)] + [h2_s[...], last_s[...]]
        for i, x in enumerate(panels):
            sum_s[2 * t + i * d : 2 * t + (i + 1) * d, :] += _cols_dot(a, x)

        @pl.when(layer > 0)
        def _():
            da = sum(_rows_dot(x, _panel(first_ref, i * d)) for i, x in enumerate(panels))
            back = _norm_back(da.astype(jnp.bfloat16).astype(jnp.float32), wide, scale)
            by_s[rows, :] = (by_s[rows, :].astype(jnp.float32) + back).astype(jnp.bfloat16)

    @pl.when(step == pl.num_programs(1) - 1)
    def _():
        events[-1]()
        pl.when(layer > 0)(lambda: _tell(n, after_free))
        per = d // n
        for i in range(own_s.shape[1] // per):
            own_s[:, i * per : (i + 1) * per, :] = sum_s[2 * t + i * d : 2 * t + (i + 1) * d, :].reshape(n, per, d).astype(jnp.bfloat16)

    @pl.when((step == pl.num_programs(1) - 1) & (layer == 0))
    def _():
        pl.when(place > 0)(lambda: _told(own_free))
        _all(scatter_events(own_s, before_ref.at[0], scratch[cut:]))


def backward(kept, dy, cos, sin, number, bq=256, bt=512):
    (layers, t, nq), nk, d = kept["q"].shape, kept["k"].shape[2], dy.shape[1]
    n = kept["tall"].shape[1]
    tokens, queries = t // bt, t // bq
    heads = nq // HEAD
    after, own = kept["tall"].shape[2] + kept["wide"].shape[2], kept["first"].shape[2]
    low, full = jnp.bfloat16, jnp.float32
    of = lambda p: layers - 1 - p
    early = lambda c: pl.BlockSpec((1, bt, c), lambda p, s: (of(p), jnp.minimum(s, tokens - 1), 0))
    late = lambda s: jnp.maximum(s - tokens - queries, 0)
    whole = lambda name: pl.BlockSpec((1, *kept[name].shape[1:]), lambda p, s: (of(p), *(0,) * (kept[name].ndim - 1)), pipeline_mode=pl.Buffered(1))
    turns = pl.BlockSpec((bt, HEAD), lambda p, s: (late(s), 0))
    names = ("mid", "o", None, "tall", "wide", "q", "k", "v", "lse", "inp", None, None, "first")
    specs = [early(d), early(nq), pl.BlockSpec((bt, d), lambda p, s: (jnp.minimum(s + p * tokens, tokens - 1), 0), pipeline_mode=pl.Buffered(1)), whole("tall"), whole("wide"),
             pl.BlockSpec((1, bq, nq), lambda p, s: (of(p), jnp.clip(s - tokens, 0, queries - 1), 0)), whole("k"), whole("v"), whole("lse"),
             pl.BlockSpec((1, bt, d), lambda p, s: (of(p), late(s), 0)), turns, turns, whole("first")]
    others = iter((dy, cos, sin))
    outs = [(layers, after, d), (layers, own, d)]
    buffers = [((t, d), low), ((t, nq), low), ((bt, d), low), ((bt, d), low), ((heads, HEAD, bq), full), ((heads, t), full), ((2 * t + nq + 2 * nk, d), full),
               ((n, after, d), low), ((n, own, d), low)]
    return pl.pallas_call(
        functools.partial(_backward, bq=bq, bt=bt),
        grid=(layers, 2 * tokens + queries),
        in_specs=specs,
        out_specs=[pl.BlockSpec((1, after, d), lambda p, s: (of(p), 0, 0), pipeline_mode=pl.Buffered(1)), _whole(outs[1])],
        out_shape=[jax.ShapeDtypeStruct(x, low) for x in outs],
        scratch_shapes=[*[pltpu.VMEM(*b) for b in buffers], *[pltpu.SemaphoreType.REGULAR] * 2, *scatter_scratch(n, after, d), *scatter_scratch(n, own, d)],
        compiler_params=_params(2, **_talks(number)),
        name="backward",
        cost_estimate=pl.CostEstimate(flops=layers * 30 * t * t * nq, transcendentals=t * t * heads, bytes_accessed=t * nq * 20),
    )(*[kept[name] if name else next(others) for name in names])


def _adamw(*refs, places):
    count = len(places)
    cut = len(refs) - 6 * count
    grads, rest = refs[:cut], refs[cut:]
    threes = [rest[i : i + 3] for i in range(0, len(rest), 3)]
    for (block, at), given, new in zip(places, threes[:count], threes[count:], strict=True):
        d = grads[block].shape[2]
        _, rows, cols = given[0].shape
        for c in range(0, cols, d):
            g = grads[block][0, at : at + rows, :].astype(jnp.float32)
            at += rows
            w, m, v = (ref[0, :, c : c + d] for ref in given)
            w = w.astype(jnp.float32)
            m = 0.9 * m + 0.1 * g
            v = 0.95 * v + 0.05 * g * g
            step = m * lax.rsqrt(v + 1e-8) + 0.1 * w
            for ref, value in zip(new, ((w - 0.02 * step).astype(jnp.bfloat16), m, v), strict=True):
                ref[0, :, c : c + d] = value


def adamw(grads, given):
    places, flat = [], []
    for block, some in enumerate(given):
        at = 0
        for three in some:
            places.append((block, at))
            at += three[0][0].size // grads[block].shape[2]
            flat += three
    each = lambda x: pl.BlockSpec((1, *x.shape[1:]), lambda i: (i, 0, 0))
    size = sum(x.size for x in flat) // 3
    out = pl.pallas_call(
        functools.partial(_adamw, places=places),
        grid=flat[0].shape[:1],
        in_specs=[each(x) for x in (*grads, *flat)],
        out_specs=[each(x) for x in flat],
        out_shape=[jax.ShapeDtypeStruct(x.shape, x.dtype) for x in flat],
        compiler_params=_params(1),
        name="adamw",
        cost_estimate=pl.CostEstimate(flops=15 * size, transcendentals=size, bytes_accessed=22 * size),
    )(*grads, *flat)
    return [out[i : i + 3] for i in range(0, len(out), 3)]


def solution(mesh):
    n = mesh.shape["dp"]

    def step(x, dy, *arrays):
        w, m, v = (dict(zip(NAMES, arrays[i : i + 7], strict=True)) for i in (0, 7, 14))
        kept, cos, sin = forward(x[0], w, n, 1)
        order = [_names(TALL + WIDE), _names(FIRST)]
        got = adamw(backward(kept, dy[0], cos, sin, 2), [[(w[name], m[name], v[name]) for name in names] for names in order])
        new = dict(zip(sum(order, []), got, strict=True))
        return tuple(new[name][which] for which in range(3) for name in NAMES)

    states, cut = P(("rep", "dp"), None, None), P(None, "dp", None)
    return jax.shard_map(
        step,
        mesh=mesh,
        in_specs=(states, states) + (cut,) * 21,
        out_specs=(P("rep", "dp", None),) * 21,
        check_vma=False,
    )
```
